32 devices in a mesh: share: 4 (over z), row: 8 (over y, x, core).
Axes of the slice: x: 2, y: 2, z: 4, core: 2. Of those that a mesh axis runs over, the one named last changes fastest.
Arguments:
- remaining_coded_pieces: float32 [16, 128, 8192], P('share', 'row'), may hold values from -6 to 6
- alive_piece_indices: int32 [16], replicated, may hold values from 0 to 19, as said below
- slab_starting_positions: int32 [2], replicated, may hold values from 0 to 48
Outputs:
- decoded: float32 [16, 128, 4096], P('share', None, 'row')
The draws below stay inside these ranges and needn't reach their ends.
Inputs may be any that keep to these rules, and one draw needn't show every extreme that they name: `alive_piece_indices`: 16 different share numbers in rising order.
All inputs are finite; a program needn't handle non-finite values.
Results may differ from the reference program's by a relative error of at most 0.00007.
Values sent between devices are 32-bit elements; how exact they have to be, the bound alone decides.
No kernel may reach another device: no remote copies, remote signals or barrier semaphores. Data moves between devices by JAX's collectives and lax.ppermute only.
A program may use at most 64 MiB of HBM per device.

```python
import jax
import jax.numpy as jnp
from jax import lax

K = 16
CODED_PIECES_ALL = 20
W = 2048
COLS = 8192
R_WIN = 128


def draw_alive_piece_indices(key, part):
    shuffled = jax.random.permutation(jax.random.fold_in(key, 7), CODED_PIECES_ALL)
    return jnp.sort(shuffled[:K]).astype(jnp.int32)


def block_scale(stream_key, dims, split, least, top_value):
    def one(dim, blocks):
        draws = jax.random.uniform(jax.random.fold_in(jax.random.fold_in(stream_key, 6), dim), (blocks,), jnp.float32, least / len(split), top_value / len(split))
        return jnp.repeat(jnp.exp(draws), dims[dim] // blocks).reshape((-1,) + (1,) * (len(dims) - dim - 1))

    level = one(*split[0])
    for cut in split[1:]:
        level = level * one(*cut)
    return level


def noise(stream_key, extent, deviation, limit, cuts=(), held_as=jnp.bfloat16):
    level = block_scale(stream_key, extent, cuts, -0.22, 0.18) if cuts else 1.0
    values = jax.random.normal(stream_key, extent, jnp.float32) * deviation * level
    return jnp.minimum(jnp.maximum(values, -limit), limit).astype(held_as)


def setup_inputs(seed: int = 0) -> dict:
    keys = jax.random.split(jax.random.key(seed), 4)
    remaining_coded_pieces = noise(keys[0], (K, R_WIN, COLS), 1.0, 6.0, ((0, 4), (1, 8)), jnp.float32)
    alive_piece_indices = draw_alive_piece_indices(jax.random.fold_in(keys[3], 71), 0)
    slab_starting_positions = jax.random.randint(keys[2], (2,), 0, (COLS - W) // 128 + 1).astype(jnp.int32)
    return dict(remaining_coded_pieces=remaining_coded_pieces, alive_piece_indices=alive_piece_indices, slab_starting_positions=slab_starting_positions)


def recovery_operator(alive_piece_indices):
    numbers = jnp.arange(CODED_PIECES_ALL, dtype=jnp.float32)
    nodes = jnp.cos(jnp.pi * (2.0 * numbers + 1.0) / (2.0 * CODED_PIECES_ALL))
    chosen_coded_pieces = (alive_piece_indices[:, None] == jnp.arange(CODED_PIECES_ALL, dtype=jnp.int32)[None, :]).astype(jnp.float32)
    points = jnp.sum(chosen_coded_pieces * nodes[None, :], axis=1)
    polynomial_degrees = jnp.arange(K, dtype=jnp.float32)
    angles = jnp.pi * (2.0 * polynomial_degrees + 1.0) / (2.0 * K)
    samples = jnp.cos(angles)
    same = jnp.arange(K, dtype=jnp.int32)[:, None] == jnp.arange(K, dtype=jnp.int32)[None, :]
    spacing = jnp.where(same, 1.0, points[:, None] - points[None, :])
    factors = (samples[None, None, :] - points[None, :, None]) / spacing[:, :, None]
    factors = jnp.where(same[:, :, None], 1.0, factors)
    lagrange = jnp.prod(factors, axis=1)
    table = jnp.cos(polynomial_degrees[:, None] * angles[None, :])
    recovery_coefficients = (2.0 / K) * jnp.sum(table[:, None, :] * lagrange[None, :, :], axis=2)
    return recovery_coefficients * jnp.where(polynomial_degrees == 0.0, 0.5, 1.0)[:, None]


def reference(remaining_coded_pieces, alive_piece_indices, slab_starting_positions):
    recovery_coefficients = recovery_operator(alive_piece_indices)
    first = lax.dynamic_slice_in_dim(remaining_coded_pieces, (slab_starting_positions[0] * 128).astype(jnp.int32), W, 2)
    second = lax.dynamic_slice_in_dim(remaining_coded_pieces, (slab_starting_positions[1] * 128).astype(jnp.int32), W, 2)
    slabs = jnp.concatenate([first, second], axis=2)
    return jnp.einsum("ki,irc->krc", recovery_coefficients, slabs, precision=lax.Precision.HIGHEST)
```

```python
import jax
import jax.numpy as jnp
from jax import lax
from jax.sharding import PartitionSpec as P

K = 16
CODED_PIECES_ALL = 20
W = 2048


def recovery_operator(alive_piece_indices):
    numbers = jnp.arange(CODED_PIECES_ALL, dtype=jnp.float32)
    nodes = jnp.cos(jnp.pi * (2.0 * numbers + 1.0) / (2.0 * CODED_PIECES_ALL))
    chosen_coded_pieces = (
        alive_piece_indices[:, None] == jnp.arange(CODED_PIECES_ALL, dtype=jnp.int32)[None, :]
    ).astype(jnp.float32)
    points = jnp.sum(chosen_coded_pieces * nodes[None, :], axis=1)
    polynomial_degrees = jnp.arange(K, dtype=jnp.float32)
    angles = jnp.pi * (2.0 * polynomial_degrees + 1.0) / (2.0 * K)
    samples = jnp.cos(angles)
    same = jnp.arange(K, dtype=jnp.int32)[:, None] == jnp.arange(K, dtype=jnp.int32)[None, :]
    spacing = jnp.where(same, 1.0, points[:, None] - points[None, :])
    factors = (samples[None, None, :] - points[None, :, None]) / spacing[:, :, None]
    factors = jnp.where(same[:, :, None], 1.0, factors)
    lagrange = jnp.prod(factors, axis=1)
    table = jnp.cos(polynomial_degrees[:, None] * angles[None, :])
    recovery_coefficients = 2.0 / K * jnp.sum(table[:, None, :] * lagrange[None, :, :], axis=2)
    return recovery_coefficients * jnp.where(polynomial_degrees == 0.0, 0.5, 1.0)[:, None]


def solution(mesh):
    shares, rows = mesh.shape["share"], mesh.shape["row"]

    def body(pieces, alive, starts):
        weights = recovery_operator(alive)
        held, depth, _ = pieces.shape
        width = 2 * W // rows
        part = width // shares
        slabs = jnp.concatenate(
            [lax.dynamic_slice_in_dim(pieces, starts[n] * 128, W, 2) for n in range(2)], axis=2
        )
        sent = slabs.reshape(held, depth, rows, shares, part).transpose(3, 2, 0, 1, 4)
        got = lax.all_to_all(sent, "share", split_axis=0, concat_axis=0, tiled=True)
        mixed = jnp.einsum(
            "qtsi,soirc->qotrc",
            weights.reshape(shares, K // shares, shares, held),
            got,
            precision=lax.Precision.HIGHEST,
        )
        flat = mixed.reshape(shares * rows, K // shares, depth, part)
        back = lax.all_to_all(flat, ("share", "row"), split_axis=0, concat_axis=0, tiled=True)
        back = back.reshape(shares, rows, K // shares, depth, part).transpose(2, 1, 3, 0, 4)
        return back.reshape(K // shares, rows * depth, width)

    placed = (P("share", "row", None), P(), P())
    return jax.shard_map(
        body, mesh=mesh, in_specs=placed, out_specs=P("share", None, "row"), check_vma=False
    )
```

```python
import functools

import jax
import jax.numpy as jnp
from jax import lax
from jax.experimental import pallas as pl
from jax.experimental.pallas import tpu as pltpu
from jax.sharding import PartitionSpec as P

K = 16
CODED_PIECES_ALL = 20
W = 2048

VMEM = pl.BlockSpec(memory_space=pltpu.VMEM)
SMEM = pl.BlockSpec(memory_space=pltpu.SMEM)
ANY = pl.BlockSpec(memory_space=pl.ANY)


def recovery_operator(alive_piece_indices):
    numbers = jnp.arange(CODED_PIECES_ALL, dtype=jnp.float32)
    nodes = jnp.cos(jnp.pi * (2.0 * numbers + 1.0) / (2.0 * CODED_PIECES_ALL))
    chosen_coded_pieces = (
        alive_piece_indices[:, None] == jnp.arange(CODED_PIECES_ALL, dtype=jnp.int32)[None, :]
    ).astype(jnp.float32)
    points = jnp.sum(chosen_coded_pieces * nodes[None, :], axis=1)
    polynomial_degrees = jnp.arange(K, dtype=jnp.float32)
    angles = jnp.pi * (2.0 * polynomial_degrees + 1.0) / (2.0 * K)
    samples = jnp.cos(angles)
    same = jnp.arange(K, dtype=jnp.int32)[:, None] == jnp.arange(K, dtype=jnp.int32)[None, :]
    spacing = jnp.where(same, 1.0, points[:, None] - points[None, :])
    factors = (samples[None, None, :] - points[None, :, None]) / spacing[:, :, None]
    factors = jnp.where(same[:, :, None], 1.0, factors)
    lagrange = jnp.prod(factors, axis=1)
    table = jnp.cos(polynomial_degrees[:, None] * angles[None, :])
    recovery_coefficients = 2.0 / K * jnp.sum(table[:, None, :] * lagrange[None, :, :], axis=2)
    return recovery_coefficients * jnp.where(polynomial_degrees == 0.0, 0.5, 1.0)[:, None]


class Sizes:
    def __init__(self, mesh, pieces):
        self.shares, self.rows = mesh.shape["share"], mesh.shape["row"]
        self.held = pieces[0] // self.shares
        self.depth = pieces[1] // self.rows
        self.kept = K // self.shares
        self.half = self.depth // 2
        self.width = 2 * W // self.rows
        self.part = self.width // self.shares

    def tiled(self):
        powers = all(n & (n - 1) == 0 for n in (self.shares, self.rows))
        whole = self.depth % 16 == 0 and self.width % (128 * self.shares) == 0
        return powers and whole and W % self.width == 0


def floats(*shape):
    return jax.ShapeDtypeStruct(shape, jnp.float32)


def params(mib):
    return pltpu.CompilerParams(vmem_limit_bytes=mib << 20)


def cost(words, flops=0):
    return pl.CostEstimate(flops=flops or words, bytes_accessed=4 * words, transcendentals=0)


def run(copies):
    for copy in copies:
        copy.start()
    for copy in copies:
        copy.wait()


def first_column(z, starts, row):
    slab = (row * z.width) // W
    return starts[slab] * 128 + row * z.width - slab * W


def share_cut(z, starts, pieces, *refs):
    outs, sems = refs[:-1], refs[-1]
    share, row = lax.axis_index("share"), lax.axis_index("row")
    copies = []
    for m in range(z.shares):
        for p in range(z.rows):
            column = first_column(z, starts, row ^ p) + (share ^ m) * z.part
            copies.append(
                pltpu.make_async_copy(
                    pieces.at[:, pl.ds(0, z.half), pl.ds(pl.multiple_of(column, 128), z.part)],
                    outs[m].at[p],
                    sems.at[m, p],
                )
            )
    run(copies)


def row_cut(z, starts, pieces, *refs):
    outs, sems = refs[:-1], refs[-1]
    row = lax.axis_index("row")
    copies = []
    for p in range(z.rows):
        column = first_column(z, starts, row ^ p)
        copies.append(
            pltpu.make_async_copy(
                pieces.at[:, pl.ds(z.half, z.half), pl.ds(pl.multiple_of(column, 128), z.width)],
                outs[p],
                sems.at[p],
            )
        )
    run(copies)


def rows_to_shares(z, *refs):
    ins, outs = refs[: z.rows], refs[z.rows :]
    share = lax.axis_index("share")
    for m in range(z.shares):
        column = pl.multiple_of((share ^ m) * z.part, 128)
        for p in range(z.rows):
            outs[m][p] = ins[p][:, :, pl.ds(column, z.part)]


def shares_to_rows(z, *refs):
    ins, outs = refs[: z.shares], refs[z.shares :]
    for m in range(z.shares):
        for p in range(z.rows):
            outs[p][m] = ins[m][p]


def mix(z, weights, *refs):
    ins, outs = refs[: z.shares], refs[z.shares :]
    share = lax.axis_index("share")
    for m in range(z.shares):
        for k in range(z.kept):
            total = None
            for n in range(z.shares):
                for i in range(z.held):
                    weight = weights[(share ^ m) * z.kept + k, (share ^ n) * z.held + i]
                    term = weight * ins[n][:, i]
                    total = term if total is None else total + term
            outs[m][:, k] = total


def place_upper(z, *refs):
    ins, out, sems = refs[: z.rows], refs[z.rows], refs[z.rows + 1]
    place(z, out, sems, 0, lambda p, m: ins[p].at[m])


def place_lower(z, *refs):
    ins, out, sems = refs[1 : z.shares + 1], refs[z.shares + 1], refs[z.shares + 2]
    place(z, out, sems, z.half, lambda p, m: ins[m].at[p])


def place(z, out, sems, first, source):
    share, row = lax.axis_index("share"), lax.axis_index("row")
    copies = []
    for p in range(z.rows):
        for m in range(z.shares):
            line = pl.multiple_of((row ^ p) * z.depth + first, 8)
            column = pl.multiple_of((share ^ m) * z.part, 128)
            copies.append(
                pltpu.make_async_copy(
                    source(p, m),
                    out.at[:, pl.ds(line, z.half), pl.ds(column, z.part)],
                    sems.at[p, m],
                )
            )
    run(copies)


def exchange(arrays, axis, peers):
    return [
        lax.ppermute(array, axis, [(i, i ^ m) for i in range(peers)]) if m else array
        for m, array in reversed(list(enumerate(arrays)))
    ][::-1]


def plain_body(z, pieces, alive, starts):
    weights = recovery_operator(alive)
    slabs = jnp.concatenate(
        [lax.dynamic_slice_in_dim(pieces, starts[n] * 128, W, 2) for n in range(2)], axis=2
    )
    sent = slabs.reshape(z.held, z.depth, z.rows, z.shares, z.part).transpose(3, 2, 0, 1, 4)
    got = lax.all_to_all(sent, "share", split_axis=0, concat_axis=0, tiled=True)
    mixed = jnp.einsum(
        "qtsi,soirc->qotrc",
        weights.reshape(z.shares, z.kept, z.shares, z.held),
        got,
        precision=lax.Precision.HIGHEST,
    )
    flat = mixed.reshape(z.shares * z.rows, z.kept, z.depth, z.part)
    back = lax.all_to_all(flat, ("share", "row"), split_axis=0, concat_axis=0, tiled=True)
    back = back.reshape(z.shares, z.rows, z.kept, z.depth, z.part).transpose(2, 1, 3, 0, 4)
    return back.reshape(z.kept, z.rows * z.depth, z.width)


def tiled_body(z, pieces, alive, starts):
    weights = recovery_operator(alive)
    words = z.shares * z.rows * z.held * z.half * z.part
    slots = floats(z.rows, z.held, z.half, z.part)
    blocks = floats(z.rows, z.kept, z.half, z.part)

    def call(kernel, name, outs, ins, scratch=(), flops=0, **more):
        return pl.pallas_call(
            functools.partial(kernel, z),
            out_shape=outs,
            scratch_shapes=scratch,
            compiler_params=params(8),
            cost_estimate=cost(2 * words, flops),
            name=name,
            **more,
        )(*ins)

    def cut(kernel, name, outs, *sems):
        return call(
            kernel,
            name,
            outs,
            (starts, pieces),
            [pltpu.SemaphoreType.DMA(sems)],
            in_specs=[SMEM, ANY],
            out_specs=[VMEM] * len(outs),
        )

    def decode(name, arrays):
        return call(
            mix,
            name,
            [blocks] * z.shares,
            (weights, *arrays),
            flops=2 * K * words,
            in_specs=[SMEM] + [VMEM] * z.shares,
            out_specs=[VMEM] * z.shares,
        )

    upper = cut(share_cut, "share_cut", [slots] * z.shares, z.shares, z.rows)
    upper = exchange(upper, "share", z.shares)
    lower = cut(row_cut, "row_cut", [floats(z.held, z.half, z.width)] * z.rows, z.rows)
    lower = exchange(lower, "row", z.rows)
    lower = call(
        rows_to_shares,
        "rows_to_shares",
        [slots] * z.shares,
        lower,
        in_specs=[VMEM] * z.rows,
        out_specs=[VMEM] * z.shares,
    )
    lower = exchange(lower, "share", z.shares)
    upper = exchange(decode("mix_upper", upper), "share", z.shares)
    lower = exchange(decode("mix_lower", lower), "share", z.shares)
    upper = call(
        shares_to_rows,
        "shares_to_rows",
        [floats(z.shares, z.kept, z.half, z.part)] * z.rows,
        upper,
        in_specs=[VMEM] * z.shares,
        out_specs=[VMEM] * z.rows,
    )
    upper = exchange(upper, "row", z.rows)
    sems = [pltpu.SemaphoreType.DMA((z.rows, z.shares))]
    out = floats(z.kept, z.rows * z.depth, z.width)
    out_upper = call(
        place_upper, "place_upper", out, upper, sems, in_specs=[VMEM] * z.rows, out_specs=ANY
    )
    return call(
        place_lower,
        "place_lower",
        out,
        (out_upper, *lower),
        sems,
        in_specs=[ANY] + [VMEM] * z.shares,
        out_specs=ANY,
        input_output_aliases={0: 0},
    )


def solution(mesh):
    def body(pieces, alive, starts):
        shape = (
            pieces.shape[0] * mesh.shape["share"],
            pieces.shape[1] * mesh.shape["row"],
            pieces.shape[2],
        )
        z = Sizes(mesh, shape)
        return (tiled_body if z.tiled() else plain_body)(z, pieces, alive, starts)

    placed = (P("share", "row", None), P(), P())
    return jax.shard_map(
        body, mesh=mesh, in_specs=placed, out_specs=P("share", None, "row"), check_vma=False
    )
```

```python
import functools

import jax
import jax.numpy as jnp
from jax import lax
from jax.experimental import pallas as pl
from jax.experimental.pallas import tpu as pltpu
from jax.sharding import PartitionSpec as P

K = 16
CODED_PIECES_ALL = 20
W = 2048

VMEM = pl.BlockSpec(memory_space=pltpu.VMEM)
SMEM = pl.BlockSpec(memory_space=pltpu.SMEM)
ANY = pl.BlockSpec(memory_space=pl.ANY)


def recovery_operator(alive_piece_indices):
    numbers = jnp.arange(CODED_PIECES_ALL, dtype=jnp.float32)
    nodes = jnp.cos(jnp.pi * (2.0 * numbers + 1.0) / (2.0 * CODED_PIECES_ALL))
    chosen_coded_pieces = (
        alive_piece_indices[:, None] == jnp.arange(CODED_PIECES_ALL, dtype=jnp.int32)[None, :]
    ).astype(jnp.float32)
    points = jnp.sum(chosen_coded_pieces * nodes[None, :], axis=1)
    polynomial_degrees = jnp.arange(K, dtype=jnp.float32)
    angles = jnp.pi * (2.0 * polynomial_degrees + 1.0) / (2.0 * K)
    samples = jnp.cos(angles)
    same = jnp.arange(K, dtype=jnp.int32)[:, None] == jnp.arange(K, dtype=jnp.int32)[None, :]
    spacing = jnp.where(same, 1.0, points[:, None] - points[None, :])
    factors = (samples[None, None, :] - points[None, :, None]) / spacing[:, :, None]
    factors = jnp.where(same[:, :, None], 1.0, factors)
    lagrange = jnp.prod(factors, axis=1)
    table = jnp.cos(polynomial_degrees[:, None] * angles[None, :])
    recovery_coefficients = 2.0 / K * jnp.sum(table[:, None, :] * lagrange[None, :, :], axis=2)
    return recovery_coefficients * jnp.where(polynomial_degrees == 0.0, 0.5, 1.0)[:, None]


class Hops:
    def __init__(self, mesh):
        self.shares, self.rows = mesh.shape["share"], mesh.shape["row"]
        self.share_hops = [0, *range(self.shares - 1, 0, -1)]
        self.row_hops = [0, *range(self.rows - 1, 0, -1)]


class Sizes(Hops):
    def __init__(self, mesh, pieces):
        super().__init__(mesh)
        self.held, self.depth, _ = pieces.shape
        self.kept = K // self.shares
        self.half = self.depth // 2
        self.width = 2 * W // self.rows
        self.part = self.width // self.shares

    def tiled(self):
        powers = all(n & (n - 1) == 0 for n in (self.shares, self.rows))
        whole = self.depth % 16 == 0 and self.width % (128 * self.shares) == 0
        return powers and whole and W % self.width == 0


def floats(*shape):
    return jax.ShapeDtypeStruct(shape, jnp.float32)


def params(mib):
    return pltpu.CompilerParams(vmem_limit_bytes=mib << 20)


def cost(words, flops=0):
    return pl.CostEstimate(flops=flops or words, bytes_accessed=4 * words, transcendentals=0)


def run(copies):
    for copy in copies:
        copy.start()
    for copy in copies:
        copy.wait()


def cut(z, starts, pieces, *refs):
    upper, lower = refs[: z.shares], refs[z.shares : z.shares + z.rows]
    firsts, columns, sems = refs[z.shares + z.rows :]
    share, row = lax.axis_index("share"), lax.axis_index("row")
    copies = [pltpu.make_async_copy(starts, firsts, sems.at[0])]
    for n in range(2):
        lines = pl.ds(n * z.half, z.half)
        copies.append(pltpu.make_async_copy(pieces.at[:, lines], columns.at[n], sems.at[n + 1]))
    for copy in copies:
        copy.start()
    copies[0].wait()
    bases = []
    for p in z.row_hops:
        owner = row ^ p
        slab = (owner * z.width) // W
        bases.append(firsts[slab] * 128 + owner * z.width - slab * W)
    copies[1].wait()
    for m, hop in enumerate(z.share_hops):
        for p in range(z.rows):
            column = pl.multiple_of(bases[p] + (share ^ hop) * z.part, 128)
            upper[m][p] = columns[0, :, :, pl.ds(column, z.part)]
    copies[2].wait()
    for p in range(z.rows):
        lower[p][...] = columns[1, :, :, pl.ds(pl.multiple_of(bases[p], 128), z.width)]


def rows_to_shares(z, *refs):
    ins, outs = refs[: z.rows], refs[z.rows :]
    share = lax.axis_index("share")
    for m, hop in enumerate(z.share_hops):
        column = pl.multiple_of((share ^ hop) * z.part, 128)
        for p in range(z.rows):
            outs[m][p] = ins[p][:, :, pl.ds(column, z.part)]


def shares_to_rows(z, *refs):
    ins, outs = refs[: z.shares], refs[z.shares :]
    for m in range(z.shares):
        for p in range(z.rows):
            outs[p][m] = ins[m][p]


def mix(z, weights, *refs):
    ins, outs = refs[: z.shares], refs[z.shares :]
    share = lax.axis_index("share")
    for m, target in enumerate(z.share_hops):
        for k in range(z.kept):
            total = None
            for n, source in enumerate(z.share_hops):
                for i in range(z.held):
                    weight = weights[(share ^ target) * z.kept + k, (share ^ source) * z.held + i]
                    term = weight * ins[n][:, i]
                    total = term if total is None else total + term
            outs[m][:, k] = total


def place_upper(z, *refs):
    ins, out, sems = refs[: z.rows], refs[z.rows], refs[z.rows + 1]
    place(z, out, sems, 0, lambda p, m: ins[p].at[m])


def place_lower(z, *refs):
    ins, out, sems = refs[1 : z.shares + 1], refs[z.shares + 1], refs[z.shares + 2]
    place(z, out, sems, z.half, lambda p, m: ins[m].at[p])


def place(z, out, sems, first, source):
    share, row = lax.axis_index("share"), lax.axis_index("row")
    copies = []
    for p, row_hop in enumerate(z.row_hops):
        for m, share_hop in enumerate(z.share_hops):
            line = pl.multiple_of((row ^ row_hop) * z.depth + first, 8)
            column = pl.multiple_of((share ^ share_hop) * z.part, 128)
            copies.append(
                pltpu.make_async_copy(
                    source(p, m),
                    out.at[:, pl.ds(line, z.half), pl.ds(column, z.part)],
                    sems.at[p, m],
                )
            )
    run(copies)


def exchange(arrays, axis, hops):
    peers = range(len(hops))
    out = []
    for array, hop in zip(arrays, hops, strict=True):
        out.append(lax.ppermute(array, axis, [(i, i ^ hop) for i in peers]) if hop else array)
    return out


def plain_body(z, pieces, alive, starts):
    weights = recovery_operator(alive)
    slabs = jnp.concatenate(
        [lax.dynamic_slice_in_dim(pieces, starts[n] * 128, W, 2) for n in range(2)], axis=2
    )
    sent = slabs.reshape(z.held, z.depth, z.rows, z.shares, z.part).transpose(3, 2, 0, 1, 4)
    got = lax.all_to_all(sent, "share", split_axis=0, concat_axis=0, tiled=True)
    mixed = jnp.einsum(
        "qtsi,soirc->qotrc",
        weights.reshape(z.shares, z.kept, z.shares, z.held),
        got,
        precision=lax.Precision.HIGHEST,
    )
    flat = mixed.reshape(z.shares * z.rows, z.kept, z.depth, z.part)
    back = lax.all_to_all(flat, ("share", "row"), split_axis=0, concat_axis=0, tiled=True)
    back = back.reshape(z.shares, z.rows, z.kept, z.depth, z.part).transpose(2, 1, 3, 0, 4)
    return back.reshape(z.kept, z.rows * z.depth, z.width)


def tiled_body(z, pieces, alive, starts):
    weights = recovery_operator(alive)
    pieces = pltpu.with_memory_space_constraint(pieces, pltpu.HBM)
    words = z.shares * z.rows * z.held * z.half * z.part
    slots = floats(z.rows, z.held, z.half, z.part)
    blocks = floats(z.rows, z.kept, z.half, z.part)

    def call(kernel, outs, ins, scratch=(), flops=0, **more):
        return pl.pallas_call(
            functools.partial(kernel, z),
            out_shape=outs,
            scratch_shapes=scratch,
            compiler_params=params(8),
            cost_estimate=cost(2 * words, flops),
            **more,
        )(*ins)

    def decode(arrays):
        return call(
            mix,
            [blocks] * z.shares,
            (weights, *arrays),
            flops=2 * K * words,
            in_specs=[SMEM] + [VMEM] * z.shares,
            out_specs=[VMEM] * z.shares,
        )

    first = call(
        cut,
        [slots] * z.shares + [floats(z.held, z.half, z.width)] * z.rows,
        (pltpu.with_memory_space_constraint(starts, pltpu.HBM), pieces),
        [
            pltpu.SMEM((2,), jnp.int32),
            pltpu.VMEM((2, z.held, z.half, pieces.shape[2]), jnp.float32),
            pltpu.SemaphoreType.DMA((3,)),
        ],
        in_specs=[ANY, ANY],
        out_specs=[VMEM] * (z.shares + z.rows),
    )
    upper = exchange(first[: z.shares], "share", z.share_hops)
    lower = first[z.shares :]
    lower = exchange(lower, "row", z.row_hops)
    lower = call(
        rows_to_shares,
        [slots] * z.shares,
        lower,
        in_specs=[VMEM] * z.rows,
        out_specs=[VMEM] * z.shares,
    )
    lower = exchange(lower, "share", z.share_hops)
    upper = exchange(decode(upper), "share", z.share_hops)
    lower = exchange(decode(lower), "share", z.share_hops)
    upper = call(
        shares_to_rows,
        [floats(z.shares, z.kept, z.half, z.part)] * z.rows,
        upper,
        in_specs=[VMEM] * z.shares,
        out_specs=[VMEM] * z.rows,
    )
    upper = exchange(upper, "row", z.row_hops)
    sems = [pltpu.SemaphoreType.DMA((z.rows, z.shares))]
    out = floats(z.kept, z.rows * z.depth, z.width)
    out_upper = call(place_upper, out, upper, sems, in_specs=[VMEM] * z.rows, out_specs=ANY)
    return call(
        place_lower,
        out,
        (out_upper, *lower),
        sems,
        in_specs=[ANY] + [VMEM] * z.shares,
        out_specs=ANY,
        input_output_aliases={0: 0},
    )


def solution(mesh):
    def body(pieces, alive, starts):
        z = Sizes(mesh, pieces)
        if not z.tiled():
            return plain_body(z, pieces, alive, starts)
        return tiled_body(z, pieces, alive, starts)

    placed = (P("share", "row", None), P(), P())
    return jax.shard_map(
        body, mesh=mesh, in_specs=placed, out_specs=P("share", None, "row"), check_vma=False
    )
```

```python
import functools
import math

import jax
import jax.numpy as jnp
from jax import lax
from jax.experimental import pallas as pl
from jax.experimental.pallas import tpu as pltpu
from jax.sharding import PartitionSpec as P

K = 16
CODED_PIECES_ALL = 20
W = 2048

VMEM = pl.BlockSpec(memory_space=pltpu.VMEM)
SMEM = pl.BlockSpec(memory_space=pltpu.SMEM)
ANY = pl.BlockSpec(memory_space=pl.ANY)


def recovery_operator(alive_piece_indices):
    numbers = jnp.arange(CODED_PIECES_ALL, dtype=jnp.float32)
    nodes = jnp.cos(jnp.pi * (2.0 * numbers + 1.0) / (2.0 * CODED_PIECES_ALL))
    chosen_coded_pieces = (
        alive_piece_indices[:, None] == jnp.arange(CODED_PIECES_ALL, dtype=jnp.int32)[None, :]
    ).astype(jnp.float32)
    points = jnp.sum(chosen_coded_pieces * nodes[None, :], axis=1)
    polynomial_degrees = jnp.arange(K, dtype=jnp.float32)
    angles = jnp.pi * (2.0 * polynomial_degrees + 1.0) / (2.0 * K)
    samples = jnp.cos(angles)
    same = jnp.arange(K, dtype=jnp.int32)[:, None] == jnp.arange(K, dtype=jnp.int32)[None, :]
    spacing = jnp.where(same, 1.0, points[:, None] - points[None, :])
    factors = (samples[None, None, :] - points[None, :, None]) / spacing[:, :, None]
    factors = jnp.where(same[:, :, None], 1.0, factors)
    lagrange = jnp.prod(factors, axis=1)
    table = jnp.cos(polynomial_degrees[:, None] * angles[None, :])
    recovery_coefficients = 2.0 / K * jnp.sum(table[:, None, :] * lagrange[None, :, :], axis=2)
    return recovery_coefficients * jnp.where(polynomial_degrees == 0.0, 0.5, 1.0)[:, None]


class Hops:
    def __init__(self, mesh):
        self.shares, self.rows = mesh.shape["share"], mesh.shape["row"]
        self.share = [0, *range(self.shares - 1, 0, -1)]
        hops = range(self.rows)
        self.near = [hop for hop in hops if hop.bit_count() <= 1]
        self.far = [hop for hop in hops if hop.bit_count() > 1]


class Sizes:
    def __init__(self, mesh, pieces):
        self.shares, self.rows = mesh.shape["share"], mesh.shape["row"]
        self.held, self.depth, self.columns = pieces.shape
        self.kept = K // self.shares
        self.width = 2 * W // self.rows
        self.part = self.width // self.shares

    def tiled(self):
        powers = all(n & (n - 1) == 0 for n in (self.shares, self.rows)) and self.rows > 2
        whole = self.depth % 8 == 0 and self.width % (128 * self.shares) == 0
        return powers and whole and W % self.width == 0


def floats(*shape):
    return jax.ShapeDtypeStruct(shape, jnp.float32)


def cut(z, hops, starts, pieces, *refs):
    near, far = refs[: z.shares], refs[z.shares : z.shares + len(hops.far)]
    firsts, columns, sems = refs[z.shares + len(hops.far) :]
    share, row = lax.axis_index("share"), lax.axis_index("row")
    copies = [pltpu.make_async_copy(starts, firsts, sems.at[0])]
    for n in range(z.held):
        copies.append(pltpu.make_async_copy(pieces.at[n], columns.at[n], sems.at[n + 1]))
    for copy in copies:
        copy.start()
    copies[0].wait()

    def part(p, m):
        owner = row ^ p
        slab = (owner * z.width) // W
        first = firsts[slab] * 128 + owner * z.width - slab * W + (share ^ m) * z.part
        return columns[:, :, pl.ds(pl.multiple_of(first, 128), z.part)]

    for copy in copies[1:]:
        copy.wait()
    for m, share_hop in enumerate(hops.share):
        for p, row_hop in enumerate(hops.near):
            near[m][p] = part(row_hop, share_hop)
    for p, row_hop in enumerate(hops.far):
        for m, share_hop in enumerate(hops.share):
            far[p][m] = part(row_hop, share_hop)


def regroup(z, hops, *refs):
    outs, ins = refs[-z.shares :], refs[: -z.shares]
    for m in range(z.shares):
        for p, sent in enumerate(ins):
            outs[m][p] = sent[m]


def mix(z, hops, by_row, weights, *refs):
    ins, outs = refs[: z.shares], refs[z.shares :]
    share = lax.axis_index("share")
    for m, target in enumerate(hops.share):
        totals = [None] * z.kept
        for n, source in enumerate(hops.share):
            for i in range(z.held):
                values = ins[n][:, i]
                for k in range(z.kept):
                    weight = weights[(share ^ target) * z.kept + k, (share ^ source) * z.held + i]
                    term = weight * values
                    totals[k] = term if totals[k] is None else totals[k] + term
        for k, total in enumerate(totals):
            if by_row:
                for p, out in enumerate(outs):
                    out[m, k] = total[p]
            else:
                outs[m][:, k] = total


def place(z, hops, rows, *refs):
    ins, out, sems = refs[-z.shares - 2 : -2], refs[-2], refs[-1]
    share, row = lax.axis_index("share"), lax.axis_index("row")
    copies = []
    for m, share_hop in enumerate(hops.share):
        for p, row_hop in enumerate(rows):
            line = pl.multiple_of((row ^ row_hop) * z.depth, 8)
            column = pl.multiple_of((share ^ share_hop) * z.part, 128)
            there = out.at[:, pl.ds(line, z.depth), pl.ds(column, z.part)]
            copies.append(pltpu.make_async_copy(ins[m].at[p], there, sems.at[m, p]))
    for copy in copies:
        copy.start()
    for copy in copies:
        copy.wait()


def exchange(arrays, axis, peers, hops):
    out = []
    for array, hop in zip(arrays, hops, strict=True):
        pairs = [(i, i ^ hop) for i in range(peers)]
        out.append(lax.ppermute(array, axis, pairs) if hop else array)
    return out


def plain_body(z, pieces, alive, starts):
    weights = recovery_operator(alive)
    slabs = jnp.concatenate(
        [lax.dynamic_slice_in_dim(pieces, starts[n] * 128, W, 2) for n in range(2)], axis=2
    )
    sent = slabs.reshape(z.held, z.depth, z.rows, z.shares, z.part).transpose(3, 2, 0, 1, 4)
    got = lax.all_to_all(sent, "share", split_axis=0, concat_axis=0, tiled=True)
    mixed = jnp.einsum(
        "qtsi,soirc->qotrc",
        weights.reshape(z.shares, z.kept, z.shares, z.held),
        got,
        precision=lax.Precision.HIGHEST,
    )
    flat = mixed.reshape(z.shares * z.rows, z.kept, z.depth, z.part)
    back = lax.all_to_all(flat, ("share", "row"), split_axis=0, concat_axis=0, tiled=True)
    back = back.reshape(z.shares, z.rows, z.kept, z.depth, z.part).transpose(2, 1, 3, 0, 4)
    return back.reshape(z.kept, z.rows * z.depth, z.width)


def tiled_body(z, hops, pieces, alive, starts):
    weights = recovery_operator(alive)
    near, far, shares = len(hops.near), len(hops.far), z.shares

    def call(kernel, outs, ins, in_specs, out_specs, scratch=(), flops=0, **more):
        words = sum(math.prod(out.shape) for out in jax.tree.leaves(outs))
        return pl.pallas_call(
            functools.partial(kernel, z, hops),
            out_shape=outs,
            in_specs=in_specs,
            out_specs=out_specs,
            scratch_shapes=scratch,
            compiler_params=pltpu.CompilerParams(vmem_limit_bytes=8 << 20),
            cost_estimate=pl.CostEstimate(
                flops=flops or words, bytes_accessed=8 * words, transcendentals=0
            ),
            **more,
        )(*ins)

    def over_shares(arrays):
        return exchange(arrays, "share", shares, hops.share)

    def over_rows(arrays, rows):
        return exchange(arrays, "row", z.rows, rows)

    def slots(count, lead, blocks):
        return [floats(lead, blocks, z.depth, z.part)] * count

    def regrouped(arrays, blocks):
        outs = slots(shares, len(arrays), blocks)
        return call(regroup, outs, arrays, [VMEM] * len(arrays), [VMEM] * shares)

    def mixed(arrays, rows, by_row):
        outs = slots(rows, shares, z.kept) if by_row else slots(shares, rows, z.kept)
        specs = [SMEM] + [VMEM] * shares
        return call(
            lambda z, hops, *refs: mix(z, hops, by_row, *refs),
            outs,
            (weights, *arrays),
            specs,
            [VMEM] * len(outs),
            flops=2 * K * rows * K * z.depth * z.part,
        )

    def placed(arrays, rows, base=()):
        return call(
            lambda z, hops, *refs: place(z, hops, rows, *refs),
            floats(z.kept, z.rows * z.depth, z.width),
            (*base, *arrays),
            [ANY] * len(base) + [VMEM] * shares,
            ANY,
            [pltpu.SemaphoreType.DMA((shares, len(rows)))],
            input_output_aliases={0: 0} if base else {},
        )

    in_hbm = [pltpu.with_memory_space_constraint(a, pltpu.HBM) for a in (starts, pieces)]
    scratch = [
        pltpu.SMEM((2,), jnp.int32),
        pltpu.VMEM((z.held, z.depth, z.columns), jnp.float32),
        pltpu.SemaphoreType.DMA((z.held + 1,)),
    ]
    parts = slots(shares, near, z.held) + [floats(shares, z.held, z.depth, z.part)] * far
    parts = call(cut, parts, in_hbm, [ANY, ANY], [VMEM] * len(parts), scratch)
    first = over_shares(parts[:shares])
    second = over_rows(parts[shares:], hops.far)
    second = over_shares(regrouped(second, z.held))
    first = over_rows(mixed(first, near, True), hops.near)
    first = over_shares(regrouped(first, z.kept))
    second = over_shares(mixed(second, far, False))
    out = placed(first, hops.near)
    return placed(second, hops.far, (out,))


def solution(mesh):
    hops = Hops(mesh)

    def body(pieces, alive, starts):
        z = Sizes(mesh, pieces)
        if not z.tiled():
            return plain_body(z, pieces, alive, starts)
        return tiled_body(z, hops, pieces, alive, starts)

    placed = (P("share", "row", None), P(), P())
    return jax.shard_map(
        body, mesh=mesh, in_specs=placed, out_specs=P("share", None, "row"), check_vma=False
    )
```

```python
import functools
import math

import jax
import jax.numpy as jnp
from jax import lax
from jax.experimental import pallas as pl
from jax.experimental.pallas import tpu as pltpu
from jax.sharding import PartitionSpec as P

K = 16
CODED_PIECES_ALL = 20
W = 2048

VMEM = pl.BlockSpec(memory_space=pltpu.VMEM)
SMEM = pl.BlockSpec(memory_space=pltpu.SMEM)
ANY = pl.BlockSpec(memory_space=pl.ANY)


def recovery_operator(alive_piece_indices):
    numbers = jnp.arange(CODED_PIECES_ALL, dtype=jnp.float32)
    nodes = jnp.cos(jnp.pi * (2.0 * numbers + 1.0) / (2.0 * CODED_PIECES_ALL))
    chosen_coded_pieces = (
        alive_piece_indices[:, None] == jnp.arange(CODED_PIECES_ALL, dtype=jnp.int32)[None, :]
    ).astype(jnp.float32)
    points = jnp.sum(chosen_coded_pieces * nodes[None, :], axis=1)
    polynomial_degrees = jnp.arange(K, dtype=jnp.float32)
    angles = jnp.pi * (2.0 * polynomial_degrees + 1.0) / (2.0 * K)
    samples = jnp.cos(angles)
    same = jnp.arange(K, dtype=jnp.int32)[:, None] == jnp.arange(K, dtype=jnp.int32)[None, :]
    spacing = jnp.where(same, 1.0, points[:, None] - points[None, :])
    factors = (samples[None, None, :] - points[None, :, None]) / spacing[:, :, None]
    factors = jnp.where(same[:, :, None], 1.0, factors)
    lagrange = jnp.prod(factors, axis=1)
    table = jnp.cos(polynomial_degrees[:, None] * angles[None, :])
    recovery_coefficients = 2.0 / K * jnp.sum(table[:, None, :] * lagrange[None, :, :], axis=2)
    return recovery_coefficients * jnp.where(polynomial_degrees == 0.0, 0.5, 1.0)[:, None]


class Hops:
    def __init__(self, mesh):
        self.shares, self.rows = mesh.shape["share"], mesh.shape["row"]
        self.share = [0, *range(self.shares - 1, 0, -1)]
        others = range(2, self.rows)
        self.near = [0, 1]
        self.middle = [hop for hop in others if hop.bit_count() % 2 == 1]
        self.far = [hop for hop in others if hop.bit_count() % 2 == 0]


class Sizes:
    def __init__(self, mesh, pieces):
        self.shares, self.rows = mesh.shape["share"], mesh.shape["row"]
        self.held, self.depth, self.columns = pieces.shape
        self.kept = K // self.shares
        self.width = 2 * W // self.rows
        self.part = self.width // self.shares

    def tiled(self):
        powers = all(n & (n - 1) == 0 for n in (self.shares, self.rows)) and self.rows > 2
        whole = self.depth % 8 == 0 and self.width % (128 * self.shares) == 0
        return powers and whole and W % self.width == 0


def floats(*shape):
    return jax.ShapeDtypeStruct(shape, jnp.float32)


def cut(z, hops, starts, pieces, *refs):
    count = 2 * z.shares + len(hops.far)
    near, middle, far = refs[: z.shares], refs[z.shares : 2 * z.shares], refs[2 * z.shares : count]
    firsts, columns, sems = refs[count:]
    share, row = lax.axis_index("share"), lax.axis_index("row")
    copies = [pltpu.make_async_copy(starts, firsts, sems.at[0])]
    for n in range(z.held):
        copies.append(pltpu.make_async_copy(pieces.at[n], columns.at[n], sems.at[n + 1]))
    for copy in copies:
        copy.start()
    copies[0].wait()

    def part(p, m):
        owner = row ^ p
        slab = (owner * z.width) // W
        first = firsts[slab] * 128 + owner * z.width - slab * W + (share ^ m) * z.part
        return columns[:, :, pl.ds(pl.multiple_of(first, 128), z.part)]

    for copy in copies[1:]:
        copy.wait()
    for early, rows in ((near, hops.near), (middle, hops.middle)):
        for m, share_hop in enumerate(hops.share):
            for p, row_hop in enumerate(rows):
                early[m][p] = part(row_hop, share_hop)
    for p, row_hop in enumerate(hops.far):
        for m, share_hop in enumerate(hops.share):
            far[p][m] = part(row_hop, share_hop)


def regroup(z, hops, *refs):
    outs, ins = refs[-z.shares :], refs[: -z.shares]
    for m in range(z.shares):
        for p, sent in enumerate(ins):
            outs[m][p] = sent[m]


def mix(z, hops, by_row, weights, *refs):
    ins, outs = refs[: z.shares], refs[z.shares :]
    share = lax.axis_index("share")
    for m, target in enumerate(hops.share):
        totals = [None] * z.kept
        for n, source in enumerate(hops.share):
            for i in range(z.held):
                values = ins[n][:, i]
                for k in range(z.kept):
                    weight = weights[(share ^ target) * z.kept + k, (share ^ source) * z.held + i]
                    term = weight * values
                    totals[k] = term if totals[k] is None else totals[k] + term
        for k, total in enumerate(totals):
            if by_row:
                for p, out in enumerate(outs):
                    out[m, k] = total[p]
            else:
                outs[m][:, k] = total


def place(z, hops, chunks, *refs):
    ins, out, sems = refs[-len(chunks) * z.shares - 2 : -2], refs[-2], refs[-1]
    share, row = lax.axis_index("share"), lax.axis_index("row")
    copies = []
    for n, rows in enumerate(chunks):
        for m, share_hop in enumerate(hops.share):
            for p, row_hop in enumerate(rows):
                line = pl.multiple_of((row ^ row_hop) * z.depth, 8)
                column = pl.multiple_of((share ^ share_hop) * z.part, 128)
                there = out.at[:, pl.ds(line, z.depth), pl.ds(column, z.part)]
                here = ins[n * z.shares + m].at[p]
                copies.append(pltpu.make_async_copy(here, there, sems.at[len(copies)]))
    for copy in copies:
        copy.start()
    for copy in copies:
        copy.wait()


def exchange(arrays, axis, peers, hops):
    out = []
    for array, hop in zip(arrays, hops, strict=True):
        pairs = [(i, i ^ hop) for i in range(peers)]
        out.append(lax.ppermute(array, axis, pairs) if hop else array)
    return out


def plain_body(z, pieces, alive, starts):
    weights = recovery_operator(alive)
    slabs = jnp.concatenate(
        [lax.dynamic_slice_in_dim(pieces, starts[n] * 128, W, 2) for n in range(2)], axis=2
    )
    sent = slabs.reshape(z.held, z.depth, z.rows, z.shares, z.part).transpose(3, 2, 0, 1, 4)
    got = lax.all_to_all(sent, "share", split_axis=0, concat_axis=0, tiled=True)
    mixed = jnp.einsum(
        "qtsi,soirc->qotrc",
        weights.reshape(z.shares, z.kept, z.shares, z.held),
        got,
        precision=lax.Precision.HIGHEST,
    )
    flat = mixed.reshape(z.shares * z.rows, z.kept, z.depth, z.part)
    back = lax.all_to_all(flat, ("share", "row"), split_axis=0, concat_axis=0, tiled=True)
    back = back.reshape(z.shares, z.rows, z.kept, z.depth, z.part).transpose(2, 1, 3, 0, 4)
    return back.reshape(z.kept, z.rows * z.depth, z.width)


def tiled_body(z, hops, pieces, alive, starts):
    weights = recovery_operator(alive)
    shares = z.shares

    def call(kernel, outs, ins, in_specs, out_specs, scratch=(), flops=0, **more):
        words = sum(math.prod(out.shape) for out in jax.tree.leaves(outs))
        return pl.pallas_call(
            functools.partial(kernel, z, hops),
            out_shape=outs,
            in_specs=in_specs,
            out_specs=out_specs,
            scratch_shapes=scratch,
            compiler_params=pltpu.CompilerParams(vmem_limit_bytes=8 << 20),
            cost_estimate=pl.CostEstimate(
                flops=flops or words, bytes_accessed=8 * words, transcendentals=0
            ),
            **more,
        )(*ins)

    def over_shares(arrays):
        return exchange(arrays, "share", shares, hops.share)

    def over_rows(arrays, rows):
        return exchange(arrays, "row", z.rows, rows)

    def slots(count, lead, blocks):
        return [floats(lead, blocks, z.depth, z.part)] * count

    def regrouped(arrays, blocks):
        outs = slots(shares, len(arrays), blocks)
        return call(regroup, outs, arrays, [VMEM] * len(arrays), [VMEM] * shares)

    def mixed(arrays, rows, by_row):
        outs = slots(rows, shares, z.kept) if by_row else slots(shares, rows, z.kept)
        specs = [SMEM] + [VMEM] * shares
        return call(
            lambda z, hops, *refs: mix(z, hops, by_row, *refs),
            outs,
            (weights, *arrays),
            specs,
            [VMEM] * len(outs),
            flops=2 * K * rows * K * z.depth * z.part,
        )

    def placed(arrays, chunks, base=()):
        copies = shares * sum(len(rows) for rows in chunks)
        return call(
            lambda z, hops, *refs: place(z, hops, chunks, *refs),
            floats(z.kept, z.rows * z.depth, z.width),
            (*base, *arrays),
            [ANY] * len(base) + [VMEM] * len(arrays),
            ANY,
            [pltpu.SemaphoreType.DMA((copies,))],
            input_output_aliases={0: 0} if base else {},
        )

    def mixed_and_crossed(arrays, rows):
        arrays = mixed(arrays, len(rows), True)
        arrays = over_rows(arrays, rows)
        return regrouped(arrays, z.kept)

    in_hbm = [pltpu.with_memory_space_constraint(a, pltpu.HBM) for a in (starts, pieces)]
    scratch = [
        pltpu.SMEM((2,), jnp.int32),
        pltpu.VMEM((z.held, z.depth, z.columns), jnp.float32),
        pltpu.SemaphoreType.DMA((z.held + 1,)),
    ]
    parts = slots(shares, len(hops.near), z.held) + slots(shares, len(hops.middle), z.held)
    parts += slots(len(hops.far), shares, z.held)
    parts = call(cut, parts, in_hbm, [ANY, ANY], [VMEM] * len(parts), scratch)
    near = over_shares(parts[:shares])
    middle = over_shares(parts[shares : 2 * shares])
    far = over_rows(parts[2 * shares :], hops.far)
    near = over_shares(mixed_and_crossed(near, hops.near))
    far = over_shares(regrouped(far, z.held))
    middle = over_shares(mixed_and_crossed(middle, hops.middle))
    far = over_shares(mixed(far, len(hops.far), False))
    out = placed(near + middle, [hops.near, hops.middle])
    return placed(far, [hops.far], (out,))


def solution(mesh):
    hops = Hops(mesh)

    def body(pieces, alive, starts):
        z = Sizes(mesh, pieces)
        if not z.tiled():
            return plain_body(z, pieces, alive, starts)
        return tiled_body(z, hops, pieces, alive, starts)

    placed = (P("share", "row", None), P(), P())
    return jax.shard_map(
        body, mesh=mesh, in_specs=placed, out_specs=P("share", None, "row"), check_vma=False
    )
```

```python
import functools
import math

import jax
import jax.numpy as jnp
from jax import lax
from jax.experimental import pallas as pl
from jax.experimental.pallas import tpu as pltpu
from jax.sharding import PartitionSpec as P

K = 16
CODED_PIECES_ALL = 20
W = 2048

VMEM = pl.BlockSpec(memory_space=pltpu.VMEM)
SMEM = pl.BlockSpec(memory_space=pltpu.SMEM)
ANY = pl.BlockSpec(memory_space=pl.ANY)


def recovery_operator(alive_piece_indices):
    numbers = jnp.arange(CODED_PIECES_ALL, dtype=jnp.float32)
    nodes = jnp.cos(jnp.pi * (2.0 * numbers + 1.0) / (2.0 * CODED_PIECES_ALL))
    chosen_coded_pieces = (
        alive_piece_indices[:, None] == jnp.arange(CODED_PIECES_ALL, dtype=jnp.int32)[None, :]
    ).astype(jnp.float32)
    points = jnp.sum(chosen_coded_pieces * nodes[None, :], axis=1)
    polynomial_degrees = jnp.arange(K, dtype=jnp.float32)
    angles = jnp.pi * (2.0 * polynomial_degrees + 1.0) / (2.0 * K)
    samples = jnp.cos(angles)
    same = jnp.arange(K, dtype=jnp.int32)[:, None] == jnp.arange(K, dtype=jnp.int32)[None, :]
    spacing = jnp.where(same, 1.0, points[:, None] - points[None, :])
    factors = (samples[None, None, :] - points[None, :, None]) / spacing[:, :, None]
    factors = jnp.where(same[:, :, None], 1.0, factors)
    lagrange = jnp.prod(factors, axis=1)
    table = jnp.cos(polynomial_degrees[:, None] * angles[None, :])
    recovery_coefficients = 2.0 / K * jnp.sum(table[:, None, :] * lagrange[None, :, :], axis=2)
    return recovery_coefficients * jnp.where(polynomial_degrees == 0.0, 0.5, 1.0)[:, None]


class Hops:
    def __init__(self, mesh):
        self.shares, self.rows = mesh.shape["share"], mesh.shape["row"]
        self.share = [0, *range(self.shares - 1, 0, -1)]
        others = range(3, self.rows)
        self.near = [0, 1, 2]
        self.middle = [hop for hop in others if hop.bit_count() % 2 == 1]
        self.far = [hop for hop in others if hop.bit_count() % 2 == 0]


class Sizes:
    def __init__(self, mesh, pieces):
        self.shares, self.rows = mesh.shape["share"], mesh.shape["row"]
        self.held, self.depth, self.columns = pieces.shape
        self.kept = K // self.shares
        self.width = 2 * W // self.rows
        self.part = self.width // self.shares

    def tiled(self):
        powers = all(n & (n - 1) == 0 for n in (self.shares, self.rows)) and self.rows > 4
        whole = self.depth % 8 == 0 and self.width == 128 * self.shares
        return powers and whole and W % self.width == 0


def floats(*shape):
    return jax.ShapeDtypeStruct(shape, jnp.float32)


def cut(z, hops, starts, pieces, *refs):
    count = 2 * z.shares + len(hops.far)
    near, middle, far = refs[: z.shares], refs[z.shares : 2 * z.shares], refs[2 * z.shares : count]
    firsts, columns, sems = refs[count:]
    share, row = lax.axis_index("share"), lax.axis_index("row")
    copies = [pltpu.make_async_copy(starts, firsts, sems.at[0])]
    for n in range(z.held):
        copies.append(pltpu.make_async_copy(pieces.at[n], columns.at[n], sems.at[n + 1]))
    for copy in copies:
        copy.start()
    copies[0].wait()

    def part(p, m):
        owner = row ^ p
        slab = (owner * z.width) // W
        first = firsts[slab] * 128 + owner * z.width - slab * W + (share ^ m) * z.part
        return columns[:, :, pl.ds(pl.multiple_of(first, 128), z.part)]

    for copy in copies[1:]:
        copy.wait()
    for early, rows in ((near, hops.near), (middle, hops.middle)):
        for m, share_hop in enumerate(hops.share):
            for p, row_hop in enumerate(rows):
                early[m][p] = part(row_hop, share_hop)
    for p, row_hop in enumerate(hops.far):
        for m, share_hop in enumerate(hops.share):
            far[p][m] = part(row_hop, share_hop)


def regroup(z, hops, *refs):
    outs, ins = refs[-z.shares :], refs[: -z.shares]
    for m in range(z.shares):
        for p, sent in enumerate(ins):
            outs[m][p] = sent[m]


def mix(z, hops, by_row, weights, *refs):
    ins, outs, spread = refs[: z.shares], refs[z.shares : -1], refs[-1]
    share = lax.axis_index("share")
    table = weights[...]
    for i in range(K):
        spread[i] = jnp.broadcast_to(table[:, i : i + 1], (K, 128))
    for m, target in enumerate(hops.share):
        totals = [None] * z.kept
        for n, source in enumerate(hops.share):
            for i in range(z.held):
                values = ins[n][:, i]
                for k in range(z.kept):
                    line = pl.ds((share ^ target) * z.kept + k, 1)
                    term = spread[(share ^ source) * z.held + i, line] * values
                    totals[k] = term if totals[k] is None else totals[k] + term
        for k, total in enumerate(totals):
            if by_row:
                for p, out in enumerate(outs):
                    out[m, k] = total[p]
            else:
                outs[m][:, k] = total


def place(z, hops, chunks, *refs):
    ins, out, sems = refs[-len(chunks) * z.shares - 2 : -2], refs[-2], refs[-1]
    share, row = lax.axis_index("share"), lax.axis_index("row")
    copies = []
    for n, rows in enumerate(chunks):
        for m, share_hop in enumerate(hops.share):
            for p, row_hop in enumerate(rows):
                line = pl.multiple_of((row ^ row_hop) * z.depth, 8)
                column = pl.multiple_of((share ^ share_hop) * z.part, 128)
                there = out.at[:, pl.ds(line, z.depth), pl.ds(column, z.part)]
                here = ins[n * z.shares + m].at[p]
                copies.append(pltpu.make_async_copy(here, there, sems.at[len(copies)]))
    for copy in copies:
        copy.start()
    for copy in copies:
        copy.wait()


def exchange(arrays, axis, peers, hops):
    out = []
    for array, hop in zip(arrays, hops, strict=True):
        pairs = [(i, i ^ hop) for i in range(peers)]
        out.append(lax.ppermute(array, axis, pairs) if hop else array)
    return out


def plain_body(z, pieces, alive, starts):
    weights = recovery_operator(alive)
    slabs = jnp.concatenate(
        [lax.dynamic_slice_in_dim(pieces, starts[n] * 128, W, 2) for n in range(2)], axis=2
    )
    sent = slabs.reshape(z.held, z.depth, z.rows, z.shares, z.part).transpose(3, 2, 0, 1, 4)
    got = lax.all_to_all(sent, "share", split_axis=0, concat_axis=0, tiled=True)
    mixed = jnp.einsum(
        "qtsi,soirc->qotrc",
        weights.reshape(z.shares, z.kept, z.shares, z.held),
        got,
        precision=lax.Precision.HIGHEST,
    )
    flat = mixed.reshape(z.shares * z.rows, z.kept, z.depth, z.part)
    back = lax.all_to_all(flat, ("share", "row"), split_axis=0, concat_axis=0, tiled=True)
    back = back.reshape(z.shares, z.rows, z.kept, z.depth, z.part).transpose(2, 1, 3, 0, 4)
    return back.reshape(z.kept, z.rows * z.depth, z.width)


def tiled_body(z, hops, pieces, alive, starts):
    weights = recovery_operator(alive)
    shares = z.shares

    def call(kernel, outs, ins, in_specs, out_specs, scratch=(), flops=0, **more):
        words = sum(math.prod(out.shape) for out in jax.tree.leaves(outs))
        return pl.pallas_call(
            functools.partial(kernel, z, hops),
            out_shape=outs,
            in_specs=in_specs,
            out_specs=out_specs,
            scratch_shapes=scratch,
            compiler_params=pltpu.CompilerParams(vmem_limit_bytes=8 << 20),
            cost_estimate=pl.CostEstimate(
                flops=flops or words, bytes_accessed=8 * words, transcendentals=0
            ),
            **more,
        )(*ins)

    def over_shares(arrays):
        return exchange(arrays, "share", shares, hops.share)

    def over_rows(arrays, rows):
        return exchange(arrays, "row", z.rows, rows)

    def slots(count, lead, blocks):
        return [floats(lead, blocks, z.depth, z.part)] * count

    def regrouped(arrays, blocks):
        outs = slots(shares, len(arrays), blocks)
        return call(regroup, outs, arrays, [VMEM] * len(arrays), [VMEM] * shares)

    def mixed(arrays, rows, by_row):
        outs = slots(rows, shares, z.kept) if by_row else slots(shares, rows, z.kept)
        specs = [VMEM] * (1 + shares)
        return call(
            lambda z, hops, *refs: mix(z, hops, by_row, *refs),
            outs,
            (weights, *arrays),
            specs,
            [VMEM] * len(outs),
            [pltpu.VMEM((K, K, 128), jnp.float32)],
            flops=2 * K * rows * K * z.depth * z.part,
        )

    def placed(arrays, chunks, base=()):
        copies = shares * sum(len(rows) for rows in chunks)
        return call(
            lambda z, hops, *refs: place(z, hops, chunks, *refs),
            floats(z.kept, z.rows * z.depth, z.width),
            (*base, *arrays),
            [ANY] * len(base) + [VMEM] * len(arrays),
            ANY,
            [pltpu.SemaphoreType.DMA((copies,))],
            input_output_aliases={0: 0} if base else {},
        )

    def mixed_and_crossed(arrays, rows):
        arrays = mixed(arrays, len(rows), True)
        arrays = over_rows(arrays, rows)
        return regrouped(arrays, z.kept)

    in_hbm = [pltpu.with_memory_space_constraint(a, pltpu.HBM) for a in (starts, pieces)]
    scratch = [
        pltpu.SMEM((2,), jnp.int32),
        pltpu.VMEM((z.held, z.depth, z.columns), jnp.float32),
        pltpu.SemaphoreType.DMA((z.held + 1,)),
    ]
    parts = slots(shares, len(hops.near), z.held) + slots(shares, len(hops.middle), z.held)
    parts += slots(len(hops.far), shares, z.held)
    parts = call(cut, parts, in_hbm, [ANY, ANY], [VMEM] * len(parts), scratch)
    near = over_shares(parts[:shares])
    middle = over_shares(parts[shares : 2 * shares])
    far = over_rows(parts[2 * shares :], hops.far)
    far = over_shares(regrouped(far, z.held))
    near = over_shares(mixed_and_crossed(near, hops.near))
    far = over_shares(mixed(far, len(hops.far), False))
    middle = over_shares(mixed_and_crossed(middle, hops.middle))
    out = placed(near + far, [hops.near, hops.far])
    return placed(middle, [hops.middle], (out,))


def solution(mesh):
    hops = Hops(mesh)

    def body(pieces, alive, starts):
        z = Sizes(mesh, pieces)
        if not z.tiled():
            return plain_body(z, pieces, alive, starts)
        return tiled_body(z, hops, pieces, alive, starts)

    placed = (P("share", "row", None), P(), P())
    return jax.shard_map(
        body, mesh=mesh, in_specs=placed, out_specs=P("share", None, "row"), check_vma=False
    )
```

```python
import functools
import math

import jax
import jax.numpy as jnp
from jax import lax
from jax.experimental import pallas as pl
from jax.experimental.pallas import tpu as pltpu
from jax.sharding import PartitionSpec as P

K = 16
CODED_PIECES_ALL = 20
W = 2048

VMEM = pl.BlockSpec(memory_space=pltpu.VMEM)
SMEM = pl.BlockSpec(memory_space=pltpu.SMEM)
ANY = pl.BlockSpec(memory_space=pl.ANY)


def recovery_operator(alive_piece_indices):
    numbers = jnp.arange(CODED_PIECES_ALL, dtype=jnp.float32)
    nodes = jnp.cos(jnp.pi * (2.0 * numbers + 1.0) / (2.0 * CODED_PIECES_ALL))
    chosen_coded_pieces = (
        alive_piece_indices[:, None] == jnp.arange(CODED_PIECES_ALL, dtype=jnp.int32)[None, :]
    ).astype(jnp.float32)
    points = jnp.sum(chosen_coded_pieces * nodes[None, :], axis=1)
    polynomial_degrees = jnp.arange(K, dtype=jnp.float32)
    angles = jnp.pi * (2.0 * polynomial_degrees + 1.0) / (2.0 * K)
    samples = jnp.cos(angles)
    same = jnp.arange(K, dtype=jnp.int32)[:, None] == jnp.arange(K, dtype=jnp.int32)[None, :]
    spacing = jnp.where(same, 1.0, points[:, None] - points[None, :])
    factors = (samples[None, None, :] - points[None, :, None]) / spacing[:, :, None]
    factors = jnp.where(same[:, :, None], 1.0, factors)
    lagrange = jnp.prod(factors, axis=1)
    table = jnp.cos(polynomial_degrees[:, None] * angles[None, :])
    recovery_coefficients = 2.0 / K * jnp.sum(table[:, None, :] * lagrange[None, :, :], axis=2)
    return recovery_coefficients * jnp.where(polynomial_degrees == 0.0, 0.5, 1.0)[:, None]


class Hops:
    def __init__(self, mesh):
        self.shares, self.rows = mesh.shape["share"], mesh.shape["row"]
        self.share = [0, *range(self.shares - 1, 0, -1)]
        others = range(2, self.rows)
        self.near = [0, 1]
        self.middle = [hop for hop in others if hop % 2 == 1]
        self.far = [hop for hop in others if hop % 2 == 0]


class Sizes:
    def __init__(self, mesh, pieces):
        self.shares, self.rows = mesh.shape["share"], mesh.shape["row"]
        self.held, self.depth, self.columns = pieces.shape
        self.kept = K // self.shares
        self.width = 2 * W // self.rows
        self.part = self.width // self.shares

    def tiled(self):
        powers = all(n & (n - 1) == 0 for n in (self.shares, self.rows)) and self.rows > 2
        whole = self.depth % 8 == 0 and self.width == 128 * self.shares
        return powers and whole and W % self.width == 0


def floats(*shape):
    return jax.ShapeDtypeStruct(shape, jnp.float32)


def cut(z, hops, starts, pieces, *refs):
    count = 2 * z.shares + len(hops.far)
    near, middle, far = refs[: z.shares], refs[z.shares : 2 * z.shares], refs[2 * z.shares : count]
    firsts, columns, sems = refs[count:]
    share, row = lax.axis_index("share"), lax.axis_index("row")
    copies = [pltpu.make_async_copy(starts, firsts, sems.at[0])]
    for n in range(z.held):
        copies.append(pltpu.make_async_copy(pieces.at[n], columns.at[n], sems.at[n + 1]))
    for copy in copies:
        copy.start()
    copies[0].wait()

    def part(p, m):
        owner = row ^ p
        slab = (owner * z.width) // W
        first = firsts[slab] * 128 + owner * z.width - slab * W + (share ^ m) * z.part
        return columns[:, :, pl.ds(pl.multiple_of(first, 128), z.part)]

    for copy in copies[1:]:
        copy.wait()
    for early, rows in ((near, hops.near), (middle, hops.middle)):
        for m, share_hop in enumerate(hops.share):
            for p, row_hop in enumerate(rows):
                early[m][p] = part(row_hop, share_hop)
    for p, row_hop in enumerate(hops.far):
        for m, share_hop in enumerate(hops.share):
            far[p][m] = part(row_hop, share_hop)


def regroup(z, hops, *refs):
    outs, ins = refs[-z.shares :], refs[: -z.shares]
    for m in range(z.shares):
        for p, sent in enumerate(ins):
            outs[m][p] = sent[m]


def mix(z, hops, by_row, weights, *refs):
    ins, outs, spread = refs[: z.shares], refs[z.shares : -1], refs[-1]
    share = lax.axis_index("share")
    table = weights[...]
    for i in range(K):
        spread[i] = jnp.broadcast_to(table[:, i : i + 1], (K, 128))
    for m, target in enumerate(hops.share):
        totals = [None] * z.kept
        for n, source in enumerate(hops.share):
            for i in range(z.held):
                values = ins[n][:, i]
                for k in range(z.kept):
                    line = pl.ds((share ^ target) * z.kept + k, 1)
                    term = spread[(share ^ source) * z.held + i, line] * values
                    totals[k] = term if totals[k] is None else totals[k] + term
        for k, total in enumerate(totals):
            if by_row:
                for p, out in enumerate(outs):
                    out[m, k] = total[p]
            else:
                outs[m][:, k] = total


def place(z, hops, chunks, *refs):
    ins, out, sems = refs[-len(chunks) * z.shares - 2 : -2], refs[-2], refs[-1]
    share, row = lax.axis_index("share"), lax.axis_index("row")
    copies = []
    for n, rows in enumerate(chunks):
        for m, share_hop in enumerate(hops.share):
            for p, row_hop in enumerate(rows):
                line = pl.multiple_of((row ^ row_hop) * z.depth, 8)
                column = pl.multiple_of((share ^ share_hop) * z.part, 128)
                there = out.at[:, pl.ds(line, z.depth), pl.ds(column, z.part)]
                here = ins[n * z.shares + m].at[p]
                copies.append(pltpu.make_async_copy(here, there, sems.at[len(copies)]))
    for copy in copies:
        copy.start()
    for copy in copies:
        copy.wait()


def exchange(arrays, axis, peers, hops):
    out = []
    for array, hop in zip(arrays, hops, strict=True):
        pairs = [(i, i ^ hop) for i in range(peers)]
        out.append(lax.ppermute(array, axis, pairs) if hop else array)
    return out


def plain_body(z, pieces, alive, starts):
    weights = recovery_operator(alive)
    slabs = jnp.concatenate(
        [lax.dynamic_slice_in_dim(pieces, starts[n] * 128, W, 2) for n in range(2)], axis=2
    )
    sent = slabs.reshape(z.held, z.depth, z.rows, z.shares, z.part).transpose(3, 2, 0, 1, 4)
    got = lax.all_to_all(sent, "share", split_axis=0, concat_axis=0, tiled=True)
    mixed = jnp.einsum(
        "qtsi,soirc->qotrc",
        weights.reshape(z.shares, z.kept, z.shares, z.held),
        got,
        precision=lax.Precision.HIGHEST,
    )
    flat = mixed.reshape(z.shares * z.rows, z.kept, z.depth, z.part)
    back = lax.all_to_all(flat, ("share", "row"), split_axis=0, concat_axis=0, tiled=True)
    back = back.reshape(z.shares, z.rows, z.kept, z.depth, z.part).transpose(2, 1, 3, 0, 4)
    return back.reshape(z.kept, z.rows * z.depth, z.width)


def tiled_body(z, hops, pieces, alive, starts):
    weights = recovery_operator(alive)
    shares = z.shares

    def call(kernel, outs, ins, in_specs, out_specs, scratch=(), flops=0, **more):
        words = sum(math.prod(out.shape) for out in jax.tree.leaves(outs))
        return pl.pallas_call(
            functools.partial(kernel, z, hops),
            out_shape=outs,
            in_specs=in_specs,
            out_specs=out_specs,
            scratch_shapes=scratch,
            compiler_params=pltpu.CompilerParams(vmem_limit_bytes=8 << 20),
            cost_estimate=pl.CostEstimate(
                flops=flops or words, bytes_accessed=8 * words, transcendentals=0
            ),
            **more,
        )(*ins)

    def over_shares(arrays):
        return exchange(arrays, "share", shares, hops.share)

    def over_rows(arrays, rows):
        return exchange(arrays, "row", z.rows, rows)

    def slots(count, lead, blocks):
        return [floats(lead, blocks, z.depth, z.part)] * count

    def regrouped(arrays, blocks):
        outs = slots(shares, len(arrays), blocks)
        return call(regroup, outs, arrays, [VMEM] * len(arrays), [VMEM] * shares)

    def mixed(arrays, rows, by_row):
        outs = slots(rows, shares, z.kept) if by_row else slots(shares, rows, z.kept)
        specs = [VMEM] * (1 + shares)
        return call(
            lambda z, hops, *refs: mix(z, hops, by_row, *refs),
            outs,
            (weights, *arrays),
            specs,
            [VMEM] * len(outs),
            [pltpu.VMEM((K, K, 128), jnp.float32)],
            flops=2 * K * rows * K * z.depth * z.part,
        )

    def placed(arrays, chunks, base=()):
        copies = shares * sum(len(rows) for rows in chunks)
        return call(
            lambda z, hops, *refs: place(z, hops, chunks, *refs),
            floats(z.kept, z.rows * z.depth, z.width),
            (*base, *arrays),
            [ANY] * len(base) + [VMEM] * len(arrays),
            ANY,
            [pltpu.SemaphoreType.DMA((copies,))],
            input_output_aliases={0: 0} if base else {},
        )

    def mixed_and_crossed(arrays, rows):
        arrays = mixed(arrays, len(rows), True)
        arrays = over_rows(arrays, rows)
        return regrouped(arrays, z.kept)

    in_hbm = [pltpu.with_memory_space_constraint(a, pltpu.HBM) for a in (starts, pieces)]
    scratch = [
        pltpu.SMEM((2,), jnp.int32),
        pltpu.VMEM((z.held, z.depth, z.columns), jnp.float32),
        pltpu.SemaphoreType.DMA((z.held + 1,)),
    ]
    parts = slots(shares, len(hops.near), z.held) + slots(shares, len(hops.middle), z.held)
    parts += slots(len(hops.far), shares, z.held)
    parts = call(cut, parts, in_hbm, [ANY, ANY], [VMEM] * len(parts), scratch)
    near = over_shares(parts[:shares])
    middle = over_shares(parts[shares : 2 * shares])
    far = over_rows(parts[2 * shares :], hops.far)
    far = over_shares(regrouped(far, z.held))
    near = over_shares(mixed_and_crossed(near, hops.near))
    far = over_shares(mixed(far, len(hops.far), False))
    middle = over_shares(mixed_and_crossed(middle, hops.middle))
    out = placed(near + far, [hops.near, hops.far])
    return placed(middle, [hops.middle], (out,))


def solution(mesh):
    hops = Hops(mesh)

    def body(pieces, alive, starts):
        z = Sizes(mesh, pieces)
        if not z.tiled():
            return plain_body(z, pieces, alive, starts)
        return tiled_body(z, hops, pieces, alive, starts)

    placed = (P("share", "row", None), P(), P())
    return jax.shard_map(
        body, mesh=mesh, in_specs=placed, out_specs=P("share", None, "row"), check_vma=False
    )
```

```python
import functools
import math

import jax
import jax.numpy as jnp
from jax import lax
from jax.experimental import pallas as pl
from jax.experimental.pallas import tpu as pltpu
from jax.sharding import PartitionSpec as P

K = 16
CODED_PIECES_ALL = 20
W = 2048

VMEM = pl.BlockSpec(memory_space=pltpu.VMEM)
SMEM = pl.BlockSpec(memory_space=pltpu.SMEM)
ANY = pl.BlockSpec(memory_space=pl.ANY)


def recovery_operator(alive_piece_indices):
    numbers = jnp.arange(CODED_PIECES_ALL, dtype=jnp.float32)
    nodes = jnp.cos(jnp.pi * (2.0 * numbers + 1.0) / (2.0 * CODED_PIECES_ALL))
    chosen_coded_pieces = (
        alive_piece_indices[:, None] == jnp.arange(CODED_PIECES_ALL, dtype=jnp.int32)[None, :]
    ).astype(jnp.float32)
    points = jnp.sum(chosen_coded_pieces * nodes[None, :], axis=1)
    polynomial_degrees = jnp.arange(K, dtype=jnp.float32)
    angles = jnp.pi * (2.0 * polynomial_degrees + 1.0) / (2.0 * K)
    samples = jnp.cos(angles)
    same = jnp.arange(K, dtype=jnp.int32)[:, None] == jnp.arange(K, dtype=jnp.int32)[None, :]
    spacing = jnp.where(same, 1.0, points[:, None] - points[None, :])
    factors = (samples[None, None, :] - points[None, :, None]) / spacing[:, :, None]
    factors = jnp.where(same[:, :, None], 1.0, factors)
    lagrange = jnp.prod(factors, axis=1)
    table = jnp.cos(polynomial_degrees[:, None] * angles[None, :])
    recovery_coefficients = 2.0 / K * jnp.sum(table[:, None, :] * lagrange[None, :, :], axis=2)
    return recovery_coefficients * jnp.where(polynomial_degrees == 0.0, 0.5, 1.0)[:, None]


class Hops:
    def __init__(self, mesh):
        self.shares, self.rows = mesh.shape["share"], mesh.shape["row"]
        self.share = [0, *range(self.shares - 1, 0, -1)]
        self.apart = self.shares - (self.shares - 1) // 3
        others = range(2, self.rows)
        self.near = [0, 1]
        self.middle = [hop for hop in others if hop % 2 == 1]
        self.far = [hop for hop in others if hop % 2 == 0]


class Sizes:
    def __init__(self, mesh, pieces):
        self.shares, self.rows = mesh.shape["share"], mesh.shape["row"]
        self.held, self.depth, self.columns = pieces.shape
        self.kept = K // self.shares
        self.width = 2 * W // self.rows
        self.part = self.width // self.shares

    def tiled(self):
        powers = all(n & (n - 1) == 0 for n in (self.shares, self.rows)) and self.rows > 2
        whole = self.depth % 8 == 0 and self.width == 128 * self.shares
        return powers and whole and W % self.width == 0


def floats(*shape):
    return jax.ShapeDtypeStruct(shape, jnp.float32)


def cut(z, hops, starts, pieces, *refs):
    count = z.shares + hops.apart + len(hops.far)
    near, middle = refs[: z.shares], refs[z.shares : z.shares + hops.apart]
    far = refs[z.shares + hops.apart : count]
    firsts, columns, sems = refs[count:]
    share, row = lax.axis_index("share"), lax.axis_index("row")
    copies = [pltpu.make_async_copy(starts, firsts, sems.at[0])]
    for n in range(z.held):
        copies.append(pltpu.make_async_copy(pieces.at[n], columns.at[n], sems.at[n + 1]))
    for copy in copies:
        copy.start()
    copies[0].wait()

    def part(p, m):
        owner = row ^ p
        slab = (owner * z.width) // W
        first = firsts[slab] * 128 + owner * z.width - slab * W + (share ^ m) * z.part
        return columns[:, :, pl.ds(pl.multiple_of(first, 128), z.part)]

    for copy in copies[1:]:
        copy.wait()
    for m, share_hop in enumerate(hops.share):
        for p, row_hop in enumerate(hops.near):
            near[m][p] = part(row_hop, share_hop)
        for p, row_hop in enumerate(hops.middle):
            if m < hops.apart:
                middle[m][p] = part(row_hop, share_hop)
            else:
                near[m][len(hops.near) + p] = part(row_hop, share_hop)
    for p, row_hop in enumerate(hops.far):
        for m, share_hop in enumerate(hops.share):
            far[p][m] = part(row_hop, share_hop)


def regroup(z, hops, *refs):
    outs, ins = refs[-z.shares :], refs[: -z.shares]
    for m in range(z.shares):
        for p, sent in enumerate(ins):
            outs[m][p] = sent[m]


def mix(z, hops, rows, skip, by_row, weights, *refs):
    ins, outs, spread = refs[: z.shares], refs[z.shares : -1], refs[-1]
    share = lax.axis_index("share")
    table = weights[...]
    for i in range(K):
        spread[i] = jnp.broadcast_to(table[:, i : i + 1], (K, 128))
    for m, target in enumerate(hops.share):
        totals = [None] * z.kept
        for n, source in enumerate(hops.share):
            for i in range(z.held):
                first = skip if n >= hops.apart else 0
                values = ins[n][first : first + rows, i]
                for k in range(z.kept):
                    line = pl.ds((share ^ target) * z.kept + k, 1)
                    term = spread[(share ^ source) * z.held + i, line] * values
                    totals[k] = term if totals[k] is None else totals[k] + term
        for k, total in enumerate(totals):
            if by_row:
                for p, out in enumerate(outs):
                    out[m, k] = total[p]
            else:
                outs[m][:, k] = total


def place(z, hops, chunks, *refs):
    ins, out, sems = refs[-len(chunks) * z.shares - 2 : -2], refs[-2], refs[-1]
    share, row = lax.axis_index("share"), lax.axis_index("row")
    copies = []
    for n, rows in enumerate(chunks):
        for m, share_hop in enumerate(hops.share):
            for p, row_hop in enumerate(rows):
                line = pl.multiple_of((row ^ row_hop) * z.depth, 8)
                column = pl.multiple_of((share ^ share_hop) * z.part, 128)
                there = out.at[:, pl.ds(line, z.depth), pl.ds(column, z.part)]
                here = ins[n * z.shares + m].at[p]
                copies.append(pltpu.make_async_copy(here, there, sems.at[len(copies)]))
    for copy in copies:
        copy.start()
    for copy in copies:
        copy.wait()


def exchange(arrays, axis, peers, hops):
    out = []
    for array, hop in zip(arrays, hops, strict=True):
        pairs = [(i, i ^ hop) for i in range(peers)]
        out.append(lax.ppermute(array, axis, pairs) if hop else array)
    return out


def plain_body(z, pieces, alive, starts):
    weights = recovery_operator(alive)
    slabs = jnp.concatenate(
        [lax.dynamic_slice_in_dim(pieces, starts[n] * 128, W, 2) for n in range(2)], axis=2
    )
    sent = slabs.reshape(z.held, z.depth, z.rows, z.shares, z.part).transpose(3, 2, 0, 1, 4)
    got = lax.all_to_all(sent, "share", split_axis=0, concat_axis=0, tiled=True)
    mixed = jnp.einsum(
        "qtsi,soirc->qotrc",
        weights.reshape(z.shares, z.kept, z.shares, z.held),
        got,
        precision=lax.Precision.HIGHEST,
    )
    flat = mixed.reshape(z.shares * z.rows, z.kept, z.depth, z.part)
    back = lax.all_to_all(flat, ("share", "row"), split_axis=0, concat_axis=0, tiled=True)
    back = back.reshape(z.shares, z.rows, z.kept, z.depth, z.part).transpose(2, 1, 3, 0, 4)
    return back.reshape(z.kept, z.rows * z.depth, z.width)


def tiled_body(z, hops, pieces, alive, starts):
    weights = recovery_operator(alive)
    shares = z.shares

    def call(kernel, outs, ins, in_specs, out_specs, scratch=(), flops=0, **more):
        words = sum(math.prod(out.shape) for out in jax.tree.leaves(outs))
        return pl.pallas_call(
            functools.partial(kernel, z, hops),
            out_shape=outs,
            in_specs=in_specs,
            out_specs=out_specs,
            scratch_shapes=scratch,
            compiler_params=pltpu.CompilerParams(vmem_limit_bytes=8 << 20),
            cost_estimate=pl.CostEstimate(
                flops=flops or words, bytes_accessed=8 * words, transcendentals=0
            ),
            **more,
        )(*ins)

    def over_shares(arrays):
        return exchange(arrays, "share", shares, hops.share)

    def over_rows(arrays, rows):
        return exchange(arrays, "row", z.rows, rows)

    def slots(count, lead, blocks):
        return [floats(lead, blocks, z.depth, z.part)] * count

    def regrouped(arrays, blocks):
        outs = slots(shares, len(arrays), blocks)
        return call(regroup, outs, arrays, [VMEM] * len(arrays), [VMEM] * shares)

    def mixed(arrays, rows, by_row, skip=0):
        outs = slots(rows, shares, z.kept) if by_row else slots(shares, rows, z.kept)
        specs = [VMEM] * (1 + shares)
        return call(
            lambda z, hops, *refs: mix(z, hops, rows, skip, by_row, *refs),
            outs,
            (weights, *arrays),
            specs,
            [VMEM] * len(outs),
            [pltpu.VMEM((K, K, 128), jnp.float32)],
            flops=2 * K * rows * K * z.depth * z.part,
        )

    def placed(arrays, chunks, base=()):
        copies = shares * sum(len(rows) for rows in chunks)
        return call(
            lambda z, hops, *refs: place(z, hops, chunks, *refs),
            floats(z.kept, z.rows * z.depth, z.width),
            (*base, *arrays),
            [ANY] * len(base) + [VMEM] * len(arrays),
            ANY,
            [pltpu.SemaphoreType.DMA((copies,))],
            input_output_aliases={0: 0} if base else {},
        )

    def mixed_and_crossed(arrays, rows, skip=0):
        arrays = mixed(arrays, len(rows), True, skip)
        arrays = over_rows(arrays, rows)
        return regrouped(arrays, z.kept)

    in_hbm = [pltpu.with_memory_space_constraint(a, pltpu.HBM) for a in (starts, pieces)]
    scratch = [
        pltpu.SMEM((2,), jnp.int32),
        pltpu.VMEM((z.held, z.depth, z.columns), jnp.float32),
        pltpu.SemaphoreType.DMA((z.held + 1,)),
    ]
    count_near, count_middle = len(hops.near), len(hops.middle)
    parts = slots(hops.apart, count_near, z.held)
    parts += slots(shares - hops.apart, count_near + count_middle, z.held)
    parts += slots(hops.apart, count_middle, z.held) + slots(len(hops.far), shares, z.held)
    parts = call(cut, parts, in_hbm, [ANY, ANY], [VMEM] * len(parts), scratch)
    near, parts = over_shares(parts[:shares]), parts[shares:]
    middle, far = parts[: hops.apart], parts[hops.apart :]
    middle = exchange(middle, "share", shares, hops.share[: hops.apart])
    middle += near[hops.apart :]
    far = over_rows(far, hops.far)
    far = over_shares(regrouped(far, z.held))
    near = over_shares(mixed_and_crossed(near, hops.near))
    far = over_shares(mixed(far, len(hops.far), False))
    middle = over_shares(mixed_and_crossed(middle, hops.middle, count_near))
    out = placed(near + far, [hops.near, hops.far])
    return placed(middle, [hops.middle], (out,))


def solution(mesh):
    hops = Hops(mesh)

    def body(pieces, alive, starts):
        z = Sizes(mesh, pieces)
        if not z.tiled():
            return plain_body(z, pieces, alive, starts)
        return tiled_body(z, hops, pieces, alive, starts)

    placed = (P("share", "row", None), P(), P())
    return jax.shard_map(
        body, mesh=mesh, in_specs=placed, out_specs=P("share", None, "row"), check_vma=False
    )
```
